32 devices in a mesh: grp: 2 (over y), blk: 4 (over z), uly: 4 (over x, core).
Axes of the slice: x: 2, y: 2, z: 4, core: 2. Of those that a mesh axis runs over, the one named last changes fastest.
Arguments:
- qkv: bfloat16 [2, 8, 16, 3, 32, 128], P('grp', 'blk', 'uly'), parts along dimension 0, may hold values from -6 to 6
- out_weight: bfloat16 [4096, 256], replicated, may hold values from -0.25 to 0.25
- lift_weight: bfloat16 [64, 512], P(None, 'uly'), may hold values from -0.75 to 0.75
- conv_weight: bfloat16 [4, 3, 3, 512, 512], P(None, None, None, 'uly'), may hold values from -0.15625 to 0.15625
Outputs:
- pixels: bfloat16 [2, 16, 32, 512], P('grp', 'blk', None, 'uly'), parts along dimension 0
The draws below stay inside these ranges and needn't reach their ends.
There are 2 independent parts, one for each index of `grp`. The reference program is written for one: setup_inputs(seed, part) draws one part's arguments, and reference() takes and returns one part's arrays. A program takes and returns all parts, laid end to end along the dimension named above; an argument that names none is the same for every part. Nothing has to cross between parts.
All inputs are finite; a program needn't handle non-finite values.
Results may differ from the reference program's by a relative error of at most 0.02.
Values may be sent and summed in bfloat16 or wider, within the bound.
A program may use at most 64 MiB of HBM per device.

```python
import jax
import jax.numpy as jnp
from jax import lax

FRAMES = 1
HEADS = 32
HEAD = 128
PATCH = 2
LATENT = 64
CH = 512
LAYERS = 4
ROWS = 8
COLS = 16


def draw_qkv(key, part):
    shape = (FRAMES, ROWS, COLS, 3, HEADS, HEAD)
    base = jnp.clip(jax.random.normal(key, shape, jnp.float32) * 1.5, -6.0, 6.0)
    return base.astype(jnp.bfloat16)


def steps_of(stream_key, dims, pieces, least, largest):
    def one(axis_at, parts):
        draws = jax.random.uniform(jax.random.fold_in(jax.random.fold_in(stream_key, 6), axis_at), (parts,), jnp.float32, least / len(pieces), largest / len(pieces))
        return jnp.repeat(jnp.exp(draws), dims[axis_at] // parts).reshape((-1,) + (1,) * (len(dims) - axis_at - 1))

    factor_of = one(*pieces[0])
    for cut in pieces[1:]:
        factor_of = factor_of * one(*cut)
    return factor_of


def scatter_about(stream_key, dims, scale, limit, pieces=(), dtype=jnp.bfloat16):
    entries = jax.random.normal(stream_key, dims, jnp.float32) * scale
    if len(pieces) > 0:
        entries = steps_of(stream_key, dims, pieces, -0.22, 0.18) * entries
    return jnp.clip(entries, min=-limit, max=limit).astype(dtype)


def setup_inputs(seed: int = 0, part: int = 0) -> dict:
    streams_of = jax.random.split(jax.random.key(seed), 5)
    part_keys = jax.random.split(jax.random.fold_in(streams_of[4], part), 5)
    qkv = draw_qkv(jax.random.fold_in(jax.random.fold_in(streams_of[4], part), 71), part)
    out_weight = scatter_about(streams_of[1], (HEADS * HEAD, PATCH * PATCH * LATENT), (HEADS * HEAD // 8) ** -0.5, 0.25)
    lift_weight = scatter_about(streams_of[2], (LATENT, CH), LATENT ** -0.5, 0.75, ((1, 4),))
    conv_weight = scatter_about(streams_of[3], (LAYERS, 3, 3, CH, CH), (3 * CH) ** -0.5, 0.15625, ((3, 4),))
    return dict(qkv=qkv, out_weight=out_weight, lift_weight=lift_weight, conv_weight=conv_weight)


def head_attention(operands):
    queries, keys, values = operands
    scale = 1.0 / (queries.shape[-1] ** 0.5)
    scores = jnp.dot(queries.astype(jnp.float32), keys.astype(jnp.float32).T) * scale
    highest = jnp.max(scores, axis=1, keepdims=True)
    weights = jnp.exp(scores - highest)
    totals = jnp.sum(weights, axis=1, keepdims=True)
    rounded = lax.optimization_barrier(weights.astype(jnp.bfloat16))
    mixed = jnp.dot(rounded.astype(jnp.float32), values.astype(jnp.float32)) / totals
    return mixed.astype(jnp.bfloat16)


def reference(qkv, out_weight, lift_weight, conv_weight):
    frames, rows, cols = qkv.shape[0], qkv.shape[1], qkv.shape[2]
    heads, size = qkv.shape[4], qkv.shape[5]
    flat = qkv.reshape(frames * rows * cols, 3, heads, size)
    queries = jnp.transpose(flat[:, 0], (1, 0, 2))
    keys = jnp.transpose(flat[:, 1], (1, 0, 2))
    values = jnp.transpose(flat[:, 2], (1, 0, 2))
    attended = lax.map(head_attention, (queries, keys, values))
    attended = jnp.transpose(attended, (1, 0, 2)).reshape(frames * rows * cols, heads * size)
    patches = jnp.dot(attended, out_weight, preferred_element_type=jnp.float32).astype(jnp.bfloat16)
    latent_ch = lift_weight.shape[0]
    latent = patches.reshape(frames, rows, cols, PATCH, PATCH, latent_ch)
    latent = jnp.transpose(latent, (0, 1, 3, 2, 4, 5)).reshape(frames * rows * PATCH * cols * PATCH, latent_ch)
    lifted = jnp.dot(latent, lift_weight, preferred_element_type=jnp.float32).astype(jnp.bfloat16)
    channels = lift_weight.shape[1]
    current = lifted.reshape(frames, rows * PATCH, cols * PATCH, channels)
    height, width = rows * PATCH, cols * PATCH
    for layer in range(LAYERS):
        padded = jnp.pad(current, ((0, 0), (1, 1), (1, 1), (0, 0))).astype(jnp.float32)
        summed = jnp.zeros((frames, height, width, channels), jnp.float32)
        for above in range(3):
            for beside in range(3):
                window = padded[:, above:above + height, beside:beside + width, :]
                kernel = conv_weight[layer, above, beside].astype(jnp.float32)
                summed = summed + jnp.einsum("fyxc,dc->fyxd", window, kernel)
        current = jax.nn.silu(summed).astype(jnp.bfloat16)
    return current
```

```python
import functools

import jax
import jax.numpy as jnp
import numpy as np
from jax import lax
from jax.experimental import pallas as pl
from jax.experimental.pallas import tpu as pltpu
from jax.sharding import PartitionSpec as P

PATCH = 2
LAYERS = 4


def with_halo(cells, sides, width):
    for axis, dim in sides:
        count = lax.axis_size(axis)
        ends = count - 1
        head = lax.slice_in_dim(cells, 0, width, axis=dim)
        tail = lax.slice_in_dim(cells, cells.shape[dim] - width, cells.shape[dim], axis=dim)
        cells = jnp.concatenate(
            [
                lax.ppermute(tail, axis, [(i, (i + 1) % count) for i in range(ends)]),
                cells,
                lax.ppermute(head, axis, [((i + 1) % count, i) for i in range(ends)]),
            ],
            axis=dim,
        )
    return cells


def online_update(carry, pieces, start, queries, scale):
    highest, totals, summed = carry
    keys = pieces[0].reshape(-1, pieces[0].shape[-2], pieces[0].shape[-1])
    values = pieces[1].reshape(-1, pieces[1].shape[-2], pieces[1].shape[-1])
    scores = jnp.einsum("qhd,khd->hqk", queries, keys, preferred_element_type=jnp.float32) * scale
    new_high = jnp.maximum(highest, jnp.max(scores, axis=2))
    weights = jnp.exp(scores - new_high[:, :, None])
    totals = jnp.sum(weights, axis=2)
    update = jnp.einsum(
        "hqk,khd->qhd", weights.astype(jnp.bfloat16), values, preferred_element_type=jnp.float32
    )
    summed = update
    return (new_high, totals, summed)


def attention_start(flat_queries):
    count, heads, size = flat_queries.shape
    return (
        jnp.full((heads, count), -1e30, jnp.float32),
        jnp.zeros((heads, count), jnp.float32),
        jnp.zeros((count, heads, size), jnp.float32),
    )


def attention_finish(carry, shape):
    highest, totals, summed = carry
    return (summed / jnp.transpose(totals)[:, :, None]).astype(jnp.bfloat16).reshape(shape)


def unfold_patches(piece, latent_ch):
    frames, rows, cols = (piece.shape[0], piece.shape[1], piece.shape[2])
    spread = piece.reshape(frames, rows, cols, PATCH, PATCH, latent_ch)
    spread = jnp.transpose(spread, (0, 1, 3, 2, 4, 5))
    return spread.reshape(frames, rows * PATCH, cols * PATCH, latent_ch)


def conv_layer(current, kernels):
    rims = with_halo(current, (("blk", 1),), 1)
    frames, height, width, outputs = current.shape
    empty = jnp.zeros((frames, height, width, outputs), jnp.float32)
    summed = empty
    padded = jnp.pad(
        lax.all_gather(rims, "uly", axis=3, tiled=True), ((0, 0), (0, 0), (1, 1), (0, 0))
    )
    for above in range(3):
        for beside in range(3):
            window = padded[:, above : above + height, beside : beside + width, :]
            summed = summed + jnp.einsum(
                "fyxc,dc->fyxd", window, kernels[above, beside], preferred_element_type=jnp.float32
            )
    return jax.nn.silu(summed).astype(jnp.bfloat16)


def body_by_steps(qkv, out_weight, lift_weight, conv_weight):
    scale = 1.0 / qkv.shape[-1] ** 0.5
    grouped = lax.all_to_all(qkv, "blk", split_axis=4, concat_axis=1, tiled=True)
    queries = grouped[:, :, :, 0]
    flat_queries = queries.reshape(-1, queries.shape[3], queries.shape[4])
    folding = functools.partial(online_update, queries=flat_queries, scale=scale)
    carry = folding(
        attention_start(flat_queries),
        (
            lax.all_gather(grouped[:, :, :, 1], "uly", axis=2, tiled=True),
            lax.all_gather(grouped[:, :, :, 2], "uly", axis=2, tiled=True),
        ),
        jnp.int32(0),
    )
    attended = attention_finish(carry, queries.shape)
    restored = lax.all_to_all(attended, "blk", split_axis=1, concat_axis=3, tiled=True)
    frames, rows, cols = (restored.shape[0], restored.shape[1], restored.shape[2])
    features = restored.reshape(frames, rows, cols, restored.shape[3] * restored.shape[4])
    patches = jnp.einsum(
        "frcw,wp->frcp", features, out_weight, preferred_element_type=jnp.float32
    ).astype(jnp.bfloat16)
    latent_ch = lift_weight.shape[0]
    latent = unfold_patches(lax.all_gather(patches, "uly", axis=2, tiled=True), latent_ch)
    current = jnp.einsum(
        "fyxe,ed->fyxd", latent, lift_weight, preferred_element_type=jnp.float32
    ).astype(jnp.bfloat16)
    for layer in range(LAYERS):
        current = conv_layer(current, conv_weight[layer])
    return current


MESH = pl.DeviceIdType.MESH
NT = (((1,), (1,)), ((), ()))


def remote(src, dst, send, recv, target):
    return pltpu.make_async_remote_copy(
        src_ref=src, dst_ref=dst, send_sem=send, recv_sem=recv, device_id=target, device_id_type=MESH
    )


def fused_kernel(
    cfg, qkv, out_w, lift_w, conv_w, sel, keep, out,
    qkv_all, out_v, lift_all, conv_v, sel_v, keep_v, att_mine, att_all, patch_mine, patch_all, x0, acts,
    local_sem, q_send, q_recv, l_send, l_recv, a_send, a_recv, p_send, p_recv, c_send, c_recv,
):
    nb, nu, hp, size, own, width = cfg
    nd = nb * nu
    blk, uly = lax.axis_index("blk"), lax.axis_index("uly")
    me = blk * nu + uly
    count = qkv_all.shape[3]
    f32, bf16 = jnp.float32, jnp.bfloat16

    order = [(db, du) for db in sorted(range(nb), key=lambda d: -min(d, nb - d)) for du in range(nu) if db + du > 0]
    others = []
    for db, du in order:
        tb, tu = lax.rem(blk + db, nb), lax.rem(uly + du, nu)
        others.append((tb * nu + tu, {"blk": tb, "uly": tu}))
    peers = [lax.rem(uly + du, nu) for du in range(1, nu)]

    patch_all[...] = jnp.zeros_like(patch_all)
    barrier = pltpu.get_barrier_semaphore()
    for _, target in others:
        pl.semaphore_signal(barrier, inc=1, device_id=target, device_id_type=MESH)

    mine = pltpu.make_async_copy(qkv.at[me], qkv_all.at[me], local_sem.at[0])
    mine.start()
    lift_own = pltpu.make_async_copy(lift_w, lift_all.at[uly], local_sem.at[1])
    lift_own.start()
    loads = [
        pltpu.make_async_copy(a, b, local_sem.at[2 + i])
        for i, (a, b) in enumerate(((out_w, out_v), (sel, sel_v), (keep, keep_v)))
    ]
    conv_loads = [
        pltpu.make_async_copy(conv_w.at[layer], conv_v.at[layer], local_sem.at[5 + layer]) for layer in range(LAYERS)
    ]
    pl.semaphore_wait(barrier, nd - 1)

    sent = []
    for where, target in others:
        copy = remote(qkv.at[where], qkv_all.at[me], q_send.at[where], q_recv.at[me], target)
        copy.start()
        sent.append(copy)
    for peer in peers:
        copy = remote(lift_w, lift_all.at[uly], l_send.at[peer], l_recv.at[uly], {"uly": peer})
        copy.start()
        sent.append(copy)
    for copy in loads + conv_loads:
        copy.start()

    mine.wait()
    for where, target in others:
        remote(qkv.at[where], qkv_all.at[where], q_send.at[where], q_recv.at[where], target).wait_recv()

    scale = 1.0 / size**0.5
    for head in range(hp):
        q, k, v = (
            qkv_all[:, part, head].astype(f32).reshape(nd * count, size).astype(bf16) for part in range(3)
        )
        scores = lax.dot_general(q, k, NT, preferred_element_type=f32) * scale
        weights = jnp.exp(scores - jnp.max(scores, axis=1, keepdims=True))
        totals = jnp.sum(weights, axis=1, keepdims=True)
        mixed = jnp.dot(weights.astype(bf16), v, preferred_element_type=f32) / totals
        att_mine[:, :, head * size : (head + 1) * size] = mixed.reshape(nd, count, size).astype(bf16)

    for where, target in others:
        copy = remote(att_mine.at[where], att_all.at[me], a_send.at[where], a_recv.at[me], target)
        copy.start()
        sent.append(copy)

    for copy in loads:
        copy.wait()
    total = jnp.dot(att_mine[me], out_v[me], preferred_element_type=f32)
    for where, target in reversed(others):
        remote(att_mine.at[where], att_all.at[where], a_send.at[where], a_recv.at[where], target).wait_recv()
        total = total + jnp.dot(att_all[where], out_v[where], preferred_element_type=f32)
    patch = total.astype(bf16)
    patch_mine[...] = patch
    patch_all[1, uly] = patch

    def patch_copy(db, tu, slot, lane):
        return remote(
            patch_mine, patch_all.at[slot, lane], p_send.at[db + 1, tu], p_recv.at[slot, lane],
            {"blk": blk + db, "uly": tu},
        )

    reach = ((-1, blk > 0), (1, blk < nb - 1))
    for db, inside in reach:

        @pl.when(inside)
        def _():
            for tu in range(nu):
                patch_copy(db, tu, 1 - db, uly).start()

    for peer in peers:
        copy = remote(patch_mine, patch_all.at[1, uly], p_send.at[1, peer], p_recv.at[1, uly], {"uly": peer})
        copy.start()
        sent.append(copy)
    lift_own.wait()
    for peer in peers:
        remote(lift_w, lift_all.at[peer], l_send.at[peer], l_recv.at[peer], {"uly": peer}).wait_recv()
    lift = jnp.concatenate([lift_all[u] for u in range(nu)], axis=1)
    lift = jnp.concatenate([lift] * (PATCH * PATCH), axis=0)
    for peer in peers:
        remote(
            patch_mine, patch_all.at[1, peer], p_send.at[1, peer], p_recv.at[1, peer], {"uly": peer}
        ).wait_recv()
    for db, inside in reach:

        @pl.when(inside)
        def _():
            for tu in range(nu):
                copy = patch_copy(db, tu, 1 + db, tu)
                copy.wait_recv()
                copy.wait_send()

    patches = patch_all[...].astype(f32).reshape(-1, patch_all.shape[-1]).astype(bf16)
    spread = jnp.dot(sel_v[...], patches, preferred_element_type=f32).astype(bf16) * keep_v[...]
    x0[...] = jnp.dot(spread, lift, preferred_element_type=f32).astype(bf16)

    for layer in range(LAYERS):
        edge = LAYERS - 1 - layer
        span = (own + 2 * edge) * width
        conv_loads[layer].wait()
        acc = None
        for above in range(3):
            rows = slice(above * width, above * width + span)
            if layer == 0:
                window = x0[rows, :]
            else:
                window = jnp.concatenate([acts[layer - 1][u, rows, :] for u in range(nu)], axis=1)
            part = lax.dot_general(window, conv_v[layer, above], NT, preferred_element_type=f32)
            acc = part if acc is None else acc + part
        outs = acc.shape[1] // 3
        place = lax.broadcasted_iota(jnp.int32, (span, outs), 0)
        column = place & (width - 1)
        left = jnp.where(column == 0, 0.0, pltpu.roll(acc[:, :outs], 1, 0))
        right = jnp.where(column == width - 1, 0.0, pltpu.roll(acc[:, 2 * outs :], span - 1, 0))
        z = acc[:, outs : 2 * outs] + left + right
        y = z / (1.0 + jnp.exp(-z))
        if edge == 0:
            out[...] = y.astype(bf16)
            break
        place = place + (blk * own - edge) * width
        y = jnp.where((place >= 0) & (place < nb * own * width), y, 0.0).astype(bf16)
        act = acts[layer]
        act[uly] = y
        for peer in peers:
            copy = remote(
                act.at[uly], act.at[uly], c_send.at[layer, peer], c_recv.at[layer, uly], {"uly": peer}
            )
            copy.start()
            sent.append(copy)
        for peer in peers:
            remote(
                act.at[peer], act.at[peer], c_send.at[layer, peer], c_recv.at[layer, peer], {"uly": peer}
            ).wait_recv()

    for copy in sent:
        copy.wait_send()


def spread_tables(nu, rows, cols, latent_ch):
    own = PATCH * rows
    width = PATCH * cols * nu
    y, w = np.meshgrid(np.arange(own - LAYERS, 2 * own + LAYERS), np.arange(width), indexing="ij")
    y, w = y.reshape(-1), w.reshape(-1)
    slot, row = np.divmod(y // PATCH, rows)
    lane, col = np.divmod(w // PATCH, cols)
    token = ((slot * nu + lane) * rows + row) * cols + col
    sel = token[:, None] == np.arange(3 * nu * rows * cols)[None]
    piece = (y % PATCH) * PATCH + w % PATCH
    keep = piece[:, None] == (np.arange(PATCH * PATCH * latent_ch) // latent_ch)[None]
    return jnp.asarray(sel, jnp.bfloat16), jnp.asarray(keep, jnp.bfloat16)


def body_fused(nb, nu, qkv, out_weight, lift_weight, conv_weight):
    _, rows, cols, _, heads, size = qkv.shape
    nd, count = nb * nu, rows * cols
    hp = heads // nd
    own, width = PATCH * rows, PATCH * cols * nu
    latent_ch, outs = lift_weight.shape
    channels = conv_weight.shape[4]
    feats = out_weight.shape[1]
    blocks = jnp.transpose(qkv.reshape(count, 3, nd, hp, size), (2, 1, 3, 0, 4))
    sel, keep = spread_tables(nu, rows, cols, latent_ch)
    bf16 = jnp.bfloat16
    dma = pltpu.SemaphoreType.DMA
    anywhere = pl.BlockSpec(memory_space=pl.ANY)
    pixels = pl.pallas_call(
        functools.partial(fused_kernel, (nb, nu, hp, size, own, width)),
        out_shape=jax.ShapeDtypeStruct((own * width, outs), bf16),
        in_specs=[anywhere] * 6,
        out_specs=pl.BlockSpec(memory_space=pltpu.VMEM),
        scratch_shapes=[
            pltpu.VMEM((nd, 3, hp, count, size), bf16),
            pltpu.VMEM((nd, hp * size, feats), bf16),
            pltpu.VMEM((nu, latent_ch, outs), bf16),
            pltpu.VMEM((LAYERS, 3, 3 * outs, channels), bf16),
            pltpu.VMEM(sel.shape, bf16),
            pltpu.VMEM(keep.shape, bf16),
            pltpu.VMEM((nd, count, hp * size), bf16),
            pltpu.VMEM((nd, count, hp * size), bf16),
            pltpu.VMEM((count, feats), bf16),
            pltpu.VMEM((3, nu, count, feats), bf16),
            pltpu.VMEM(((own + 2 * LAYERS) * width, channels), bf16),
            [
                pltpu.VMEM((nu, (own + 2 * (LAYERS - 1 - layer)) * width, outs), bf16)
                for layer in range(LAYERS - 1)
            ],
            dma((5 + LAYERS,)),
            dma((nd,)), dma((nd,)), dma((nu,)), dma((nu,)), dma((nd,)), dma((nd,)),
            dma((3, nu)), dma((3, nu)), dma((LAYERS - 1, nu)), dma((LAYERS - 1, nu)),
        ],
        compiler_params=pltpu.CompilerParams(
            collective_id=0, has_side_effects=True, vmem_limit_bytes=60 * 1024 * 1024
        ),
    )(
        blocks,
        out_weight.reshape(nd, hp * size, feats),
        lift_weight,
        conv_weight.reshape(LAYERS, 3, 3 * outs, channels),
        sel,
        keep,
    )
    return pixels.reshape(1, own, width, outs)


def body(nb, nu, qkv, out_weight, lift_weight, conv_weight):
    frames, rows, cols, _, heads, size = qkv.shape
    width = PATCH * cols * nu
    fits = (
        frames == 1
        and nb > 1
        and nu > 1
        and heads % (nb * nu) == 0
        and (rows * cols) % 8 == 0
        and size % 128 == 0
        and lift_weight.shape[1] % 128 == 0
        and PATCH * rows >= LAYERS
        and width % 16 == 0
        and width & (width - 1) == 0
    )
    if fits:
        return body_fused(nb, nu, qkv, out_weight, lift_weight, conv_weight)
    return body_by_steps(qkv, out_weight, lift_weight, conv_weight)


def solution(mesh):
    in_specs = (
        P("grp", "blk", "uly", None, None, None),
        P(),
        P(None, "uly"),
        P(None, None, None, "uly", None),
    )
    out_specs = P("grp", "blk", None, "uly")
    step = functools.partial(body, mesh.shape["blk"], mesh.shape["uly"])
    return jax.shard_map(step, mesh=mesh, in_specs=in_specs, out_specs=out_specs, check_vma=False)
```

```python
import functools

import jax
import jax.numpy as jnp
import numpy as np
from jax import lax
from jax.experimental import pallas as pl
from jax.experimental.pallas import tpu as pltpu
from jax.sharding import PartitionSpec as P

PATCH = 2
LAYERS = 4


def with_halo(cells, sides, width):
    for axis, dim in sides:
        count = lax.axis_size(axis)
        ends = count - 1
        head = lax.slice_in_dim(cells, 0, width, axis=dim)
        tail = lax.slice_in_dim(cells, cells.shape[dim] - width, cells.shape[dim], axis=dim)
        cells = jnp.concatenate(
            [
                lax.ppermute(tail, axis, [(i, (i + 1) % count) for i in range(ends)]),
                cells,
                lax.ppermute(head, axis, [((i + 1) % count, i) for i in range(ends)]),
            ],
            axis=dim,
        )
    return cells


def online_update(carry, pieces, start, queries, scale):
    highest, totals, summed = carry
    keys = pieces[0].reshape(-1, pieces[0].shape[-2], pieces[0].shape[-1])
    values = pieces[1].reshape(-1, pieces[1].shape[-2], pieces[1].shape[-1])
    scores = jnp.einsum("qhd,khd->hqk", queries, keys, preferred_element_type=jnp.float32) * scale
    new_high = jnp.maximum(highest, jnp.max(scores, axis=2))
    weights = jnp.exp(scores - new_high[:, :, None])
    totals = jnp.sum(weights, axis=2)
    update = jnp.einsum(
        "hqk,khd->qhd", weights.astype(jnp.bfloat16), values, preferred_element_type=jnp.float32
    )
    summed = update
    return (new_high, totals, summed)


def attention_start(flat_queries):
    count, heads, size = flat_queries.shape
    return (
        jnp.full((heads, count), -1e30, jnp.float32),
        jnp.zeros((heads, count), jnp.float32),
        jnp.zeros((count, heads, size), jnp.float32),
    )


def attention_finish(carry, shape):
    highest, totals, summed = carry
    return (summed / jnp.transpose(totals)[:, :, None]).astype(jnp.bfloat16).reshape(shape)


def unfold_patches(piece, latent_ch):
    frames, rows, cols = (piece.shape[0], piece.shape[1], piece.shape[2])
    spread = piece.reshape(frames, rows, cols, PATCH, PATCH, latent_ch)
    spread = jnp.transpose(spread, (0, 1, 3, 2, 4, 5))
    return spread.reshape(frames, rows * PATCH, cols * PATCH, latent_ch)


def conv_layer(current, kernels):
    rims = with_halo(current, (("blk", 1),), 1)
    frames, height, width, outputs = current.shape
    empty = jnp.zeros((frames, height, width, outputs), jnp.float32)
    summed = empty
    padded = jnp.pad(
        lax.all_gather(rims, "uly", axis=3, tiled=True), ((0, 0), (0, 0), (1, 1), (0, 0))
    )
    for above in range(3):
        for beside in range(3):
            window = padded[:, above : above + height, beside : beside + width, :]
            summed = summed + jnp.einsum(
                "fyxc,dc->fyxd", window, kernels[above, beside], preferred_element_type=jnp.float32
            )
    return jax.nn.silu(summed).astype(jnp.bfloat16)


def body_by_steps(qkv, out_weight, lift_weight, conv_weight):
    scale = 1.0 / qkv.shape[-1] ** 0.5
    grouped = lax.all_to_all(qkv, "blk", split_axis=4, concat_axis=1, tiled=True)
    queries = grouped[:, :, :, 0]
    flat_queries = queries.reshape(-1, queries.shape[3], queries.shape[4])
    folding = functools.partial(online_update, queries=flat_queries, scale=scale)
    carry = folding(
        attention_start(flat_queries),
        (
            lax.all_gather(grouped[:, :, :, 1], "uly", axis=2, tiled=True),
            lax.all_gather(grouped[:, :, :, 2], "uly", axis=2, tiled=True),
        ),
        jnp.int32(0),
    )
    attended = attention_finish(carry, queries.shape)
    restored = lax.all_to_all(attended, "blk", split_axis=1, concat_axis=3, tiled=True)
    frames, rows, cols = (restored.shape[0], restored.shape[1], restored.shape[2])
    features = restored.reshape(frames, rows, cols, restored.shape[3] * restored.shape[4])
    patches = jnp.einsum(
        "frcw,wp->frcp", features, out_weight, preferred_element_type=jnp.float32
    ).astype(jnp.bfloat16)
    latent_ch = lift_weight.shape[0]
    latent = unfold_patches(lax.all_gather(patches, "uly", axis=2, tiled=True), latent_ch)
    current = jnp.einsum(
        "fyxe,ed->fyxd", latent, lift_weight, preferred_element_type=jnp.float32
    ).astype(jnp.bfloat16)
    for layer in range(LAYERS):
        current = conv_layer(current, conv_weight[layer])
    return current


MESH = pl.DeviceIdType.MESH
NT = (((1,), (1,)), ((), ()))


def remote(src, dst, send, recv, target):
    return pltpu.make_async_remote_copy(
        src_ref=src, dst_ref=dst, send_sem=send, recv_sem=recv, device_id=target, device_id_type=MESH
    )


def fused_kernel(
    cfg, qkv, out_w, lift_w, conv_w, sel, keep, out,
    qkv_raw, qkv_wide, qkv_mine, qkv_all, out_v, lift_all, conv_v, sel_v, keep_v, att_mine, att_all, patch_mine, patch_all, x0, acts,
    local_sem, q_send, q_recv, l_send, l_recv, a_send, a_recv, p_send, p_recv, c_send, c_recv,
):
    nb, nu, hp, size, own, width, step = cfg
    nd = nb * nu
    blk, uly = lax.axis_index("blk"), lax.axis_index("uly")
    me = blk * nu + uly
    count = qkv_all.shape[3]
    f32, bf16 = jnp.float32, jnp.bfloat16

    order = [(db, du) for db in sorted(range(nb), key=lambda d: -min(d, nb - d)) for du in range(nu) if db + du > 0]
    others = []
    for db, du in order:
        tb, tu = lax.rem(blk + db, nb), lax.rem(uly + du, nu)
        others.append((tb * nu + tu, {"blk": tb, "uly": tu}))
    peers = [lax.rem(uly + du, nu) for du in range(1, nu)]

    raw = pltpu.make_async_copy(qkv, qkv_raw, local_sem.at[0])
    raw.start()
    patch_all[...] = jnp.zeros_like(patch_all)
    barrier = pltpu.get_barrier_semaphore()
    for _, target in others:
        pl.semaphore_signal(barrier, inc=1, device_id=target, device_id_type=MESH)

    lift_own = pltpu.make_async_copy(lift_w, lift_all.at[uly], local_sem.at[1])
    lift_own.start()
    loads = [
        pltpu.make_async_copy(a, b, local_sem.at[2 + i])
        for i, (a, b) in enumerate(((out_w, out_v), (sel, sel_v), (keep, keep_v)))
    ]
    conv_loads = [
        pltpu.make_async_copy(conv_w.at[layer], conv_v.at[layer], local_sem.at[5 + layer]) for layer in range(LAYERS)
    ]
    for copy in loads + conv_loads:
        copy.start()
    raw.wait()
    qkv_wide[...] = qkv_raw[...].astype(f32)
    heads = nd * hp
    for part in range(3):
        for head in range(heads):
            tokens = qkv_wide[pl.ds(part * heads + head, count, stride=3 * heads), :]
            qkv_mine[head // hp, part, head % hp] = tokens.astype(bf16)
    pl.semaphore_wait(barrier, nd - 1)

    sent = []
    for where, target in others:
        copy = remote(qkv_mine.at[where], qkv_all.at[me], q_send.at[where], q_recv.at[me], target)
        copy.start()
        sent.append(copy)
    for peer in peers:
        copy = remote(lift_w, lift_all.at[uly], l_send.at[peer], l_recv.at[uly], {"uly": peer})
        copy.start()
        sent.append(copy)
    qkv_all[me] = qkv_mine[me]
    for where, target in others:
        remote(qkv_mine.at[where], qkv_all.at[where], q_send.at[where], q_recv.at[where], target).wait_recv()

    scale = 1.0 / size**0.5
    for head in range(hp):
        q, k, v = (
            qkv_all[:, part, head].astype(f32).reshape(nd * count, size).astype(bf16) for part in range(3)
        )
        scores = lax.dot_general(q, k, NT, preferred_element_type=f32) * scale
        weights = jnp.exp(scores - jnp.max(scores, axis=1, keepdims=True))
        totals = jnp.sum(weights, axis=1, keepdims=True)
        mixed = jnp.dot(weights.astype(bf16), v, preferred_element_type=f32) / totals
        att_mine[:, :, head * size : (head + 1) * size] = mixed.reshape(nd, count, size).astype(bf16)

    for where, target in others:
        copy = remote(att_mine.at[where], att_all.at[me], a_send.at[where], a_recv.at[me], target)
        copy.start()
        sent.append(copy)

    for copy in loads:
        copy.wait()
    total = jnp.dot(att_mine[me], out_v[me], preferred_element_type=f32)
    for where, target in reversed(others):
        remote(att_mine.at[where], att_all.at[where], a_send.at[where], a_recv.at[where], target).wait_recv()
        total = total + jnp.dot(att_all[where], out_v[where], preferred_element_type=f32)
    patch = total.astype(bf16)
    patch_mine[...] = patch
    patch_all[1, uly] = patch

    def patch_copy(db, tu, slot, lane):
        return remote(
            patch_mine, patch_all.at[slot, lane], p_send.at[db + 1, tu], p_recv.at[slot, lane],
            {"blk": blk + db, "uly": tu},
        )

    reach = ((-1, blk > 0), (1, blk < nb - 1))
    for db, inside in reach:

        @pl.when(inside)
        def _():
            for tu in range(nu):
                patch_copy(db, tu, 1 - db, uly).start()

    for peer in peers:
        copy = remote(patch_mine, patch_all.at[1, uly], p_send.at[1, peer], p_recv.at[1, uly], {"uly": peer})
        copy.start()
        sent.append(copy)
    lift_own.wait()
    for peer in peers:
        remote(lift_w, lift_all.at[peer], l_send.at[peer], l_recv.at[peer], {"uly": peer}).wait_recv()
    lift = jnp.concatenate([lift_all[u] for u in range(nu)], axis=1)
    lift = jnp.concatenate([lift] * (PATCH * PATCH), axis=0)
    for peer in peers:
        remote(
            patch_mine, patch_all.at[1, peer], p_send.at[1, peer], p_recv.at[1, peer], {"uly": peer}
        ).wait_recv()
    for db, inside in reach:

        @pl.when(inside)
        def _():
            for tu in range(nu):
                copy = patch_copy(db, tu, 1 + db, tu)
                copy.wait_recv()
                copy.wait_send()

    patches = patch_all[...].astype(f32).reshape(-1, patch_all.shape[-1]).astype(bf16)
    spread = jnp.dot(sel_v[...], patches, preferred_element_type=f32).astype(bf16) * keep_v[...]
    x0[...] = jnp.dot(spread, lift, preferred_element_type=f32).astype(bf16)

    for layer in range(LAYERS):
        edge = LAYERS - 1 - layer
        span = step * width
        conv_loads[layer].wait()
        chunks = (own + 2 * edge) // step
        ready = 0
        for chunk in range(chunks):
            base = chunk * span
            if layer > 0:
                while ready * step < (chunk + 1) * step + 2:
                    rows = slice(ready * span, (ready + 1) * span)
                    for peer in peers:
                        part = acts[layer - 1].at[peer, rows]
                        remote(
                            part, part, c_send.at[layer - 1, ready, peer], c_recv.at[layer - 1, ready, peer],
                            {"uly": peer},
                        ).wait_recv()
                    ready += 1
            acc = None
            for above in range(3):
                rows = slice(base + above * width, base + above * width + span)
                if layer == 0:
                    window = x0[rows, :]
                else:
                    window = jnp.concatenate([acts[layer - 1][u, rows, :] for u in range(nu)], axis=1)
                part = lax.dot_general(window, conv_v[layer, above], NT, preferred_element_type=f32)
                acc = part if acc is None else acc + part
            outs = acc.shape[1] // 3
            place = lax.broadcasted_iota(jnp.int32, (span, outs), 0)
            column = place & (width - 1)
            left = jnp.where(column == 0, 0.0, pltpu.roll(acc[:, :outs], 1, 0))
            right = jnp.where(column == width - 1, 0.0, pltpu.roll(acc[:, 2 * outs :], span - 1, 0))
            z = acc[:, outs : 2 * outs] + left + right
            y = z / (1.0 + jnp.exp(-z))
            if edge == 0:
                out[base : base + span, :] = y.astype(bf16)
                continue
            place = place + (base + (blk * own - edge) * width)
            y = jnp.where((place >= 0) & (place < nb * own * width), y, 0.0).astype(bf16)
            rows = slice(base, base + span)
            acts[layer][uly, rows, :] = y
            for peer in peers:
                part = acts[layer].at[uly, rows]
                copy = remote(
                    part, part, c_send.at[layer, chunk, peer], c_recv.at[layer, chunk, uly], {"uly": peer}
                )
                copy.start()
                sent.append(copy)

    for copy in sent:
        copy.wait_send()


def spread_tables(nu, rows, cols, latent_ch):
    own = PATCH * rows
    width = PATCH * cols * nu
    y, w = np.meshgrid(np.arange(own - LAYERS, 2 * own + LAYERS), np.arange(width), indexing="ij")
    y, w = y.reshape(-1), w.reshape(-1)
    slot, row = np.divmod(y // PATCH, rows)
    lane, col = np.divmod(w // PATCH, cols)
    token = ((slot * nu + lane) * rows + row) * cols + col
    sel = token[:, None] == np.arange(3 * nu * rows * cols)[None]
    piece = (y % PATCH) * PATCH + w % PATCH
    keep = piece[:, None] == (np.arange(PATCH * PATCH * latent_ch) // latent_ch)[None]
    return jnp.asarray(sel, jnp.bfloat16), jnp.asarray(keep, jnp.bfloat16)


def body_fused(nb, nu, qkv, out_weight, lift_weight, conv_weight):
    _, rows, cols, _, heads, size = qkv.shape
    nd, count = nb * nu, rows * cols
    hp = heads // nd
    own, width = PATCH * rows, PATCH * cols * nu
    step = 2
    most = (own + 2 * LAYERS) // step
    latent_ch, outs = lift_weight.shape
    channels = conv_weight.shape[4]
    feats = out_weight.shape[1]
    tokens = qkv.reshape(count * 3 * heads, size)
    sel, keep = spread_tables(nu, rows, cols, latent_ch)
    bf16 = jnp.bfloat16
    dma = pltpu.SemaphoreType.DMA
    anywhere = pl.BlockSpec(memory_space=pl.ANY)
    pixels = pl.pallas_call(
        functools.partial(fused_kernel, (nb, nu, hp, size, own, width, step)),
        out_shape=jax.ShapeDtypeStruct((own * width, outs), bf16),
        in_specs=[anywhere] * 6,
        out_specs=pl.BlockSpec(memory_space=pltpu.VMEM),
        scratch_shapes=[
            pltpu.VMEM(tokens.shape, bf16),
            pltpu.VMEM(tokens.shape, jnp.float32),
            pltpu.VMEM((nd, 3, hp, count, size), bf16),
            pltpu.VMEM((nd, 3, hp, count, size), bf16),
            pltpu.VMEM((nd, hp * size, feats), bf16),
            pltpu.VMEM((nu, latent_ch, outs), bf16),
            pltpu.VMEM((LAYERS, 3, 3 * outs, channels), bf16),
            pltpu.VMEM(sel.shape, bf16),
            pltpu.VMEM(keep.shape, bf16),
            pltpu.VMEM((nd, count, hp * size), bf16),
            pltpu.VMEM((nd, count, hp * size), bf16),
            pltpu.VMEM((count, feats), bf16),
            pltpu.VMEM((3, nu, count, feats), bf16),
            pltpu.VMEM(((own + 2 * LAYERS) * width, channels), bf16),
            [
                pltpu.VMEM((nu, (own + 2 * (LAYERS - 1 - layer)) * width, outs), bf16)
                for layer in range(LAYERS - 1)
            ],
            dma((5 + LAYERS,)),
            dma((nd,)), dma((nd,)), dma((nu,)), dma((nu,)), dma((nd,)), dma((nd,)),
            dma((3, nu)), dma((3, nu)), dma((LAYERS - 1, most, nu)), dma((LAYERS - 1, most, nu)),
        ],
        compiler_params=pltpu.CompilerParams(
            collective_id=0, has_side_effects=True, vmem_limit_bytes=60 * 1024 * 1024
        ),
    )(
        tokens,
        out_weight.reshape(nd, hp * size, feats),
        lift_weight,
        conv_weight.reshape(LAYERS, 3, 3 * outs, channels),
        sel,
        keep,
    )
    return pixels.reshape(1, own, width, outs)


def body(nb, nu, qkv, out_weight, lift_weight, conv_weight):
    frames, rows, cols, _, heads, size = qkv.shape
    width = PATCH * cols * nu
    fits = (
        frames == 1
        and nb > 1
        and nu > 1
        and heads % (nb * nu) == 0
        and (rows * cols) % 8 == 0
        and size % 128 == 0
        and lift_weight.shape[1] % 128 == 0
        and PATCH * rows >= LAYERS
        and PATCH * rows % 2 == 0
        and width % 16 == 0
        and width & (width - 1) == 0
    )
    if fits:
        return body_fused(nb, nu, qkv, out_weight, lift_weight, conv_weight)
    return body_by_steps(qkv, out_weight, lift_weight, conv_weight)


def solution(mesh):
    in_specs = (
        P("grp", "blk", "uly", None, None, None),
        P(),
        P(None, "uly"),
        P(None, None, None, "uly", None),
    )
    out_specs = P("grp", "blk", None, "uly")
    step = functools.partial(body, mesh.shape["blk"], mesh.shape["uly"])
    return jax.shard_map(step, mesh=mesh, in_specs=in_specs, out_specs=out_specs, check_vma=False)
```

```python
import functools

import jax
import jax.numpy as jnp
import numpy as np
from jax import lax
from jax.experimental import pallas as pl
from jax.experimental.pallas import tpu as pltpu
from jax.sharding import PartitionSpec as P

PATCH = 2
LAYERS = 4


def with_halo(cells, sides, width):
    for axis, dim in sides:
        count = lax.axis_size(axis)
        ends = count - 1
        head = lax.slice_in_dim(cells, 0, width, axis=dim)
        tail = lax.slice_in_dim(cells, cells.shape[dim] - width, cells.shape[dim], axis=dim)
        cells = jnp.concatenate(
            [
                lax.ppermute(tail, axis, [(i, (i + 1) % count) for i in range(ends)]),
                cells,
                lax.ppermute(head, axis, [((i + 1) % count, i) for i in range(ends)]),
            ],
            axis=dim,
        )
    return cells


def online_update(carry, pieces, start, queries, scale):
    highest, totals, summed = carry
    keys = pieces[0].reshape(-1, pieces[0].shape[-2], pieces[0].shape[-1])
    values = pieces[1].reshape(-1, pieces[1].shape[-2], pieces[1].shape[-1])
    scores = jnp.einsum("qhd,khd->hqk", queries, keys, preferred_element_type=jnp.float32) * scale
    new_high = jnp.maximum(highest, jnp.max(scores, axis=2))
    weights = jnp.exp(scores - new_high[:, :, None])
    totals = jnp.sum(weights, axis=2)
    update = jnp.einsum(
        "hqk,khd->qhd", weights.astype(jnp.bfloat16), values, preferred_element_type=jnp.float32
    )
    summed = update
    return (new_high, totals, summed)


def attention_start(flat_queries):
    count, heads, size = flat_queries.shape
    return (
        jnp.full((heads, count), -1e30, jnp.float32),
        jnp.zeros((heads, count), jnp.float32),
        jnp.zeros((count, heads, size), jnp.float32),
    )


def attention_finish(carry, shape):
    highest, totals, summed = carry
    return (summed / jnp.transpose(totals)[:, :, None]).astype(jnp.bfloat16).reshape(shape)


def unfold_patches(piece, latent_ch):
    frames, rows, cols = (piece.shape[0], piece.shape[1], piece.shape[2])
    spread = piece.reshape(frames, rows, cols, PATCH, PATCH, latent_ch)
    spread = jnp.transpose(spread, (0, 1, 3, 2, 4, 5))
    return spread.reshape(frames, rows * PATCH, cols * PATCH, latent_ch)


def conv_layer(current, kernels):
    rims = with_halo(current, (("blk", 1),), 1)
    frames, height, width, outputs = current.shape
    empty = jnp.zeros((frames, height, width, outputs), jnp.float32)
    summed = empty
    padded = jnp.pad(
        lax.all_gather(rims, "uly", axis=3, tiled=True), ((0, 0), (0, 0), (1, 1), (0, 0))
    )
    for above in range(3):
        for beside in range(3):
            window = padded[:, above : above + height, beside : beside + width, :]
            summed = summed + jnp.einsum(
                "fyxc,dc->fyxd", window, kernels[above, beside], preferred_element_type=jnp.float32
            )
    return jax.nn.silu(summed).astype(jnp.bfloat16)


def body_by_steps(qkv, out_weight, lift_weight, conv_weight):
    scale = 1.0 / qkv.shape[-1] ** 0.5
    grouped = lax.all_to_all(qkv, "blk", split_axis=4, concat_axis=1, tiled=True)
    queries = grouped[:, :, :, 0]
    flat_queries = queries.reshape(-1, queries.shape[3], queries.shape[4])
    folding = functools.partial(online_update, queries=flat_queries, scale=scale)
    carry = folding(
        attention_start(flat_queries),
        (
            lax.all_gather(grouped[:, :, :, 1], "uly", axis=2, tiled=True),
            lax.all_gather(grouped[:, :, :, 2], "uly", axis=2, tiled=True),
        ),
        jnp.int32(0),
    )
    attended = attention_finish(carry, queries.shape)
    restored = lax.all_to_all(attended, "blk", split_axis=1, concat_axis=3, tiled=True)
    frames, rows, cols = (restored.shape[0], restored.shape[1], restored.shape[2])
    features = restored.reshape(frames, rows, cols, restored.shape[3] * restored.shape[4])
    patches = jnp.einsum(
        "frcw,wp->frcp", features, out_weight, preferred_element_type=jnp.float32
    ).astype(jnp.bfloat16)
    latent_ch = lift_weight.shape[0]
    latent = unfold_patches(lax.all_gather(patches, "uly", axis=2, tiled=True), latent_ch)
    current = jnp.einsum(
        "fyxe,ed->fyxd", latent, lift_weight, preferred_element_type=jnp.float32
    ).astype(jnp.bfloat16)
    for layer in range(LAYERS):
        current = conv_layer(current, conv_weight[layer])
    return current


MESH = pl.DeviceIdType.MESH
NT = (((1,), (1,)), ((), ()))


def remote(src, dst, send, recv, target):
    return pltpu.make_async_remote_copy(
        src_ref=src, dst_ref=dst, send_sem=send, recv_sem=recv, device_id=target, device_id_type=MESH
    )


def fused_kernel(
    cfg, qkv, out_w, lift_w, conv_w, sel, keep, out,
    qkv_raw, qkv_wide, qkv_mine, qkv_all, out_v, lift_all, conv_v, sel_v, keep_v, att_mine, att_all, patch_mine, patch_all, x0, acts,
    local_sem, q_send, q_recv, l_send, l_recv, a_send, a_recv, p_send, p_recv, c_send, c_recv, f_send,
):
    nb, nu, hp, size, own, width, step = cfg
    nd = nb * nu
    blk, uly = lax.axis_index("blk"), lax.axis_index("uly")
    me = blk * nu + uly
    count = qkv_all.shape[3]
    f32, bf16 = jnp.float32, jnp.bfloat16

    order = [(db, du) for db in sorted(range(nb), key=lambda d: -min(d, nb - d)) for du in range(nu) if db + du > 0]
    others = []
    for db, du in order:
        tb, tu = lax.rem(blk + db, nb), lax.rem(uly + du, nu)
        others.append((tb * nu + tu, {"blk": tb, "uly": tu}))
    peers = [lax.rem(uly + du, nu) for du in range(1, nu)]

    raw = pltpu.make_async_copy(qkv, qkv_raw, local_sem.at[0])
    raw.start()
    patch_all[...] = jnp.zeros_like(patch_all)
    barrier = pltpu.get_barrier_semaphore()
    for _, target in others:
        pl.semaphore_signal(barrier, inc=1, device_id=target, device_id_type=MESH)

    lift_own = pltpu.make_async_copy(lift_w, lift_all.at[uly], local_sem.at[1])
    lift_own.start()
    loads = [
        pltpu.make_async_copy(a, b, local_sem.at[2 + i])
        for i, (a, b) in enumerate(((out_w, out_v), (sel, sel_v), (keep, keep_v)))
    ]
    conv_loads = [
        pltpu.make_async_copy(conv_w.at[layer], conv_v.at[layer], local_sem.at[5 + layer]) for layer in range(LAYERS)
    ]
    for copy in loads + conv_loads:
        copy.start()
    raw.wait()
    qkv_wide[...] = qkv_raw[...].astype(f32)
    heads = nd * hp
    for part in range(3):
        for head in range(heads):
            tokens = qkv_wide[pl.ds(part * heads + head, count, stride=3 * heads), :]
            qkv_mine[head // hp, part, head % hp] = tokens.astype(bf16)
    pl.semaphore_wait(barrier, nd - 1)

    sent = []
    for where, target in others:
        copy = remote(qkv_mine.at[where], qkv_all.at[me], q_send.at[where], q_recv.at[me], target)
        copy.start()
        sent.append(copy)
    for peer in peers:
        copy = remote(lift_w, lift_all.at[uly], l_send.at[peer], l_recv.at[uly], {"uly": peer})
        copy.start()
        sent.append(copy)
    qkv_all[me] = qkv_mine[me]
    for where, target in others:
        remote(qkv_mine.at[where], qkv_all.at[where], q_send.at[where], q_recv.at[where], target).wait_recv()

    scale = 1.0 / size**0.5
    for head in range(hp):
        q, k, v = (
            qkv_all[:, part, head].astype(f32).reshape(nd * count, size).astype(bf16) for part in range(3)
        )
        scores = lax.dot_general(q, k, NT, preferred_element_type=f32) * scale
        weights = jnp.exp(scores - jnp.max(scores, axis=1, keepdims=True))
        totals = jnp.sum(weights, axis=1, keepdims=True)
        mixed = jnp.dot(weights.astype(bf16), v, preferred_element_type=f32) / totals
        att_mine[:, :, head * size : (head + 1) * size] = mixed.reshape(nd, count, size).astype(bf16)

    for where, target in others:
        copy = remote(att_mine.at[where], att_all.at[me], a_send.at[where], a_recv.at[me], target)
        copy.start()
        sent.append(copy)

    for copy in loads:
        copy.wait()
    total = jnp.dot(att_mine[me], out_v[me], preferred_element_type=f32)
    for where, target in reversed(others):
        remote(att_mine.at[where], att_all.at[where], a_send.at[where], a_recv.at[where], target).wait_recv()
        total = total + jnp.dot(att_all[where], out_v[where], preferred_element_type=f32)
    patch = total.astype(bf16)
    patch_mine[...] = patch
    patch_all[1, uly] = patch

    def patch_copy(db, tu, slot, lane):
        return remote(
            patch_mine, patch_all.at[slot, lane], p_send.at[db + 1, tu], p_recv.at[slot, lane],
            {"blk": blk + db, "uly": tu},
        )

    reach = ((-1, blk > 0), (1, blk < nb - 1))
    for db, inside in reach:

        @pl.when(inside)
        def _():
            for tu in range(nu):
                patch_copy(db, tu, 1 - db, uly).start()

    for peer in peers:
        copy = remote(patch_mine, patch_all.at[1, uly], p_send.at[1, peer], p_recv.at[1, uly], {"uly": peer})
        copy.start()
        sent.append(copy)
    lift_own.wait()
    for peer in peers:
        remote(lift_w, lift_all.at[peer], l_send.at[peer], l_recv.at[peer], {"uly": peer}).wait_recv()
    lift = jnp.concatenate([lift_all[u] for u in range(nu)], axis=1)
    lift = jnp.concatenate([lift] * (PATCH * PATCH), axis=0)
    for peer in peers:
        remote(
            patch_mine, patch_all.at[1, peer], p_send.at[1, peer], p_recv.at[1, peer], {"uly": peer}
        ).wait_recv()
    for db, inside in reach:

        @pl.when(inside)
        def _():
            for tu in range(nu):
                copy = patch_copy(db, tu, 1 + db, tu)
                copy.wait_recv()
                copy.wait_send()

    patches = patch_all[...].astype(f32).reshape(-1, patch_all.shape[-1]).astype(bf16)
    spread = jnp.dot(sel_v[...], patches, preferred_element_type=f32).astype(bf16) * keep_v[...]
    x0[...] = jnp.dot(spread, lift, preferred_element_type=f32).astype(bf16)

    span = step * width
    mate = uly + 1 - 2 * lax.rem(uly, 2)
    alike = [lax.rem(uly + du, nu) for du in range(2, nu, 2)]
    near = alike + [mate]
    far = [mate] + [lax.rem(mate + du, nu) for du in range(2, nu, 2)]

    def pass_on(layer, chunk):
        for peer in alike:
            part = acts[layer].at[peer, pl.ds(chunk * span, span)]
            remote(
                part, part, c_send.at[layer, chunk, peer], c_recv.at[layer, chunk, peer], {"uly": peer}
            ).wait_recv()
            copy = remote(
                part, part, f_send.at[chunk, peer], c_recv.at[layer, chunk, peer], {"uly": mate}
            )
            copy.start()
            sent.append(copy)

    for layer in range(LAYERS):
        edge = LAYERS - 1 - layer
        conv_loads[layer].wait()
        chunks = (own + 2 * edge) // step
        ready = passed = 0
        for chunk in range(chunks):
            base = chunk * span
            if layer > 0:
                while ready * step < (chunk + 1) * step + 2:
                    while layer == 1 and passed < min(ready + 3, chunks + 1):
                        pass_on(layer - 1, passed)
                        passed += 1
                    rows = slice(ready * span, (ready + 1) * span)
                    for peer in far if layer == 1 else peers:
                        part = acts[layer - 1].at[peer, rows]
                        remote(
                            part, part, c_send.at[layer - 1, ready, peer], c_recv.at[layer - 1, ready, peer],
                            {"uly": peer},
                        ).wait_recv()
                    ready += 1
            acc = None
            for above in range(3):
                rows = slice(base + above * width, base + above * width + span)
                if layer == 0:
                    window = x0[rows, :]
                else:
                    window = jnp.concatenate([acts[layer - 1][u, rows, :] for u in range(nu)], axis=1)
                part = lax.dot_general(window, conv_v[layer, above], NT, preferred_element_type=f32)
                acc = part if acc is None else acc + part
            outs = acc.shape[1] // 3
            place = lax.broadcasted_iota(jnp.int32, (span, outs), 0)
            column = place & (width - 1)
            left = jnp.where(column == 0, 0.0, pltpu.roll(acc[:, :outs], 1, 0))
            right = jnp.where(column == width - 1, 0.0, pltpu.roll(acc[:, 2 * outs :], span - 1, 0))
            z = acc[:, outs : 2 * outs] + left + right
            y = z / (1.0 + jnp.exp(-z))
            if edge == 0:
                out[base : base + span, :] = y.astype(bf16)
                continue
            place = place + (base + (blk * own - edge) * width)
            y = jnp.where((place >= 0) & (place < nb * own * width), y, 0.0).astype(bf16)
            rows = slice(base, base + span)
            acts[layer][uly, rows, :] = y
            for peer in near if layer == 0 else peers:
                part = acts[layer].at[uly, rows]
                copy = remote(
                    part, part, c_send.at[layer, chunk, peer], c_recv.at[layer, chunk, uly], {"uly": peer}
                )
                copy.start()
                sent.append(copy)

    for copy in sent:
        copy.wait_send()


def spread_tables(nu, rows, cols, latent_ch):
    own = PATCH * rows
    width = PATCH * cols * nu
    y, w = np.meshgrid(np.arange(own - LAYERS, 2 * own + LAYERS), np.arange(width), indexing="ij")
    y, w = y.reshape(-1), w.reshape(-1)
    slot, row = np.divmod(y // PATCH, rows)
    lane, col = np.divmod(w // PATCH, cols)
    token = ((slot * nu + lane) * rows + row) * cols + col
    sel = token[:, None] == np.arange(3 * nu * rows * cols)[None]
    piece = (y % PATCH) * PATCH + w % PATCH
    keep = piece[:, None] == (np.arange(PATCH * PATCH * latent_ch) // latent_ch)[None]
    return jnp.asarray(sel, jnp.bfloat16), jnp.asarray(keep, jnp.bfloat16)


def body_fused(nb, nu, qkv, out_weight, lift_weight, conv_weight):
    _, rows, cols, _, heads, size = qkv.shape
    nd, count = nb * nu, rows * cols
    hp = heads // nd
    own, width = PATCH * rows, PATCH * cols * nu
    step = 2
    most = (own + 2 * LAYERS) // step
    latent_ch, outs = lift_weight.shape
    channels = conv_weight.shape[4]
    feats = out_weight.shape[1]
    tokens = qkv.reshape(count * 3 * heads, size)
    sel, keep = spread_tables(nu, rows, cols, latent_ch)
    bf16 = jnp.bfloat16
    dma = pltpu.SemaphoreType.DMA
    anywhere = pl.BlockSpec(memory_space=pl.ANY)
    pixels = pl.pallas_call(
        functools.partial(fused_kernel, (nb, nu, hp, size, own, width, step)),
        out_shape=pltpu.VMEM((own * width, outs), bf16),
        in_specs=[anywhere] * 6,
        out_specs=pl.BlockSpec(memory_space=pltpu.VMEM),
        scratch_shapes=[
            pltpu.VMEM(tokens.shape, bf16),
            pltpu.VMEM(tokens.shape, jnp.float32),
            pltpu.VMEM((nd, 3, hp, count, size), bf16),
            pltpu.VMEM((nd, 3, hp, count, size), bf16),
            pltpu.VMEM((nd, hp * size, feats), bf16),
            pltpu.VMEM((nu, latent_ch, outs), bf16),
            pltpu.VMEM((LAYERS, 3, 3 * outs, channels), bf16),
            pltpu.VMEM(sel.shape, bf16),
            pltpu.VMEM(keep.shape, bf16),
            pltpu.VMEM((nd, count, hp * size), bf16),
            pltpu.VMEM((nd, count, hp * size), bf16),
            pltpu.VMEM((count, feats), bf16),
            pltpu.VMEM((3, nu, count, feats), bf16),
            pltpu.VMEM(((own + 2 * LAYERS) * width, channels), bf16),
            [
                pltpu.VMEM((nu, (own + 2 * (LAYERS - 1 - layer)) * width, outs), bf16)
                for layer in range(LAYERS - 1)
            ],
            dma((5 + LAYERS,)),
            dma((nd,)), dma((nd,)), dma((nu,)), dma((nu,)), dma((nd,)), dma((nd,)),
            dma((3, nu)), dma((3, nu)), dma((LAYERS - 1, most, nu)), dma((LAYERS - 1, most, nu)), dma((most, nu)),
        ],
        compiler_params=pltpu.CompilerParams(
            collective_id=0, has_side_effects=True, vmem_limit_bytes=60 * 1024 * 1024
        ),
    )(
        tokens,
        out_weight.reshape(nd, hp * size, feats),
        lift_weight,
        conv_weight.reshape(LAYERS, 3, 3 * outs, channels),
        sel,
        keep,
    )
    return pixels.reshape(1, own, width, outs)


def body(nb, nu, qkv, out_weight, lift_weight, conv_weight):
    frames, rows, cols, _, heads, size = qkv.shape
    width = PATCH * cols * nu
    fits = (
        frames == 1
        and nb > 1
        and nu % 2 == 0
        and heads % (nb * nu) == 0
        and (rows * cols) % 8 == 0
        and size % 128 == 0
        and lift_weight.shape[1] % 128 == 0
        and PATCH * rows >= LAYERS
        and PATCH * rows % 2 == 0
        and width % 16 == 0
        and width & (width - 1) == 0
    )
    if fits:
        return body_fused(nb, nu, qkv, out_weight, lift_weight, conv_weight)
    return body_by_steps(qkv, out_weight, lift_weight, conv_weight)


def solution(mesh):
    in_specs = (
        P("grp", "blk", "uly", None, None, None),
        P(),
        P(None, "uly"),
        P(None, None, None, "uly", None),
    )
    out_specs = P("grp", "blk", None, "uly")
    step = functools.partial(body, mesh.shape["blk"], mesh.shape["uly"])
    return jax.shard_map(step, mesh=mesh, in_specs=in_specs, out_specs=out_specs, check_vma=False)
```

```python
import functools

import jax
import jax.numpy as jnp
import numpy as np
from jax import lax
from jax.experimental import pallas as pl
from jax.experimental.pallas import tpu as pltpu
from jax.sharding import PartitionSpec as P

PATCH = 2
LAYERS = 4


def with_halo(cells, sides, width):
    for axis, dim in sides:
        count = lax.axis_size(axis)
        ends = count - 1
        head = lax.slice_in_dim(cells, 0, width, axis=dim)
        tail = lax.slice_in_dim(cells, cells.shape[dim] - width, cells.shape[dim], axis=dim)
        cells = jnp.concatenate(
            [
                lax.ppermute(tail, axis, [(i, (i + 1) % count) for i in range(ends)]),
                cells,
                lax.ppermute(head, axis, [((i + 1) % count, i) for i in range(ends)]),
            ],
            axis=dim,
        )
    return cells


def online_update(carry, pieces, start, queries, scale):
    highest, totals, summed = carry
    keys = pieces[0].reshape(-1, pieces[0].shape[-2], pieces[0].shape[-1])
    values = pieces[1].reshape(-1, pieces[1].shape[-2], pieces[1].shape[-1])
    scores = jnp.einsum("qhd,khd->hqk", queries, keys, preferred_element_type=jnp.float32) * scale
    new_high = jnp.maximum(highest, jnp.max(scores, axis=2))
    weights = jnp.exp(scores - new_high[:, :, None])
    totals = jnp.sum(weights, axis=2)
    update = jnp.einsum(
        "hqk,khd->qhd", weights.astype(jnp.bfloat16), values, preferred_element_type=jnp.float32
    )
    summed = update
    return (new_high, totals, summed)


def attention_start(flat_queries):
    count, heads, size = flat_queries.shape
    return (
        jnp.full((heads, count), -1e30, jnp.float32),
        jnp.zeros((heads, count), jnp.float32),
        jnp.zeros((count, heads, size), jnp.float32),
    )


def attention_finish(carry, shape):
    highest, totals, summed = carry
    return (summed / jnp.transpose(totals)[:, :, None]).astype(jnp.bfloat16).reshape(shape)


def unfold_patches(piece, latent_ch):
    frames, rows, cols = (piece.shape[0], piece.shape[1], piece.shape[2])
    spread = piece.reshape(frames, rows, cols, PATCH, PATCH, latent_ch)
    spread = jnp.transpose(spread, (0, 1, 3, 2, 4, 5))
    return spread.reshape(frames, rows * PATCH, cols * PATCH, latent_ch)


def conv_layer(current, kernels):
    rims = with_halo(current, (("blk", 1),), 1)
    frames, height, width, outputs = current.shape
    empty = jnp.zeros((frames, height, width, outputs), jnp.float32)
    summed = empty
    padded = jnp.pad(
        lax.all_gather(rims, "uly", axis=3, tiled=True), ((0, 0), (0, 0), (1, 1), (0, 0))
    )
    for above in range(3):
        for beside in range(3):
            window = padded[:, above : above + height, beside : beside + width, :]
            summed = summed + jnp.einsum(
                "fyxc,dc->fyxd", window, kernels[above, beside], preferred_element_type=jnp.float32
            )
    return jax.nn.silu(summed).astype(jnp.bfloat16)


def body_by_steps(qkv, out_weight, lift_weight, conv_weight):
    scale = 1.0 / qkv.shape[-1] ** 0.5
    grouped = lax.all_to_all(qkv, "blk", split_axis=4, concat_axis=1, tiled=True)
    queries = grouped[:, :, :, 0]
    flat_queries = queries.reshape(-1, queries.shape[3], queries.shape[4])
    folding = functools.partial(online_update, queries=flat_queries, scale=scale)
    carry = folding(
        attention_start(flat_queries),
        (
            lax.all_gather(grouped[:, :, :, 1], "uly", axis=2, tiled=True),
            lax.all_gather(grouped[:, :, :, 2], "uly", axis=2, tiled=True),
        ),
        jnp.int32(0),
    )
    attended = attention_finish(carry, queries.shape)
    restored = lax.all_to_all(attended, "blk", split_axis=1, concat_axis=3, tiled=True)
    frames, rows, cols = (restored.shape[0], restored.shape[1], restored.shape[2])
    features = restored.reshape(frames, rows, cols, restored.shape[3] * restored.shape[4])
    patches = jnp.einsum(
        "frcw,wp->frcp", features, out_weight, preferred_element_type=jnp.float32
    ).astype(jnp.bfloat16)
    latent_ch = lift_weight.shape[0]
    latent = unfold_patches(lax.all_gather(patches, "uly", axis=2, tiled=True), latent_ch)
    current = jnp.einsum(
        "fyxe,ed->fyxd", latent, lift_weight, preferred_element_type=jnp.float32
    ).astype(jnp.bfloat16)
    for layer in range(LAYERS):
        current = conv_layer(current, conv_weight[layer])
    return current


SPLIT = ()
MESH = pl.DeviceIdType.MESH
NT = (((1,), (1,)), ((), ()))


def remote(src, dst, send, recv, target):
    return pltpu.make_async_remote_copy(
        src_ref=src, dst_ref=dst, send_sem=send, recv_sem=recv, device_id=target, device_id_type=MESH
    )


def plan(layer, rows):
    half = rows // 2 if layer in SPLIT else rows
    return [0, half] + ([rows] if half < rows else [])


def fused_kernel(
    cfg, qkv, out_w, lift_w, conv_w, sel, keep, out,
    qkv_raw, qkv_wide, qkv_mine, qkv_all, out_v, lift_all, conv_v, sel_v, keep_v, att_mine, att_all, patch_mine, patch_all, x0, acts,
    local_sem, q_send, q_recv, l_send, l_recv, a_send, a_recv, p_send, p_recv, c_send, c_recv,
):
    nb, nu, hp, size, own, width = cfg
    nd = nb * nu
    blk, uly = lax.axis_index("blk"), lax.axis_index("uly")
    me = blk * nu + uly
    count = qkv_all.shape[3]
    f32, bf16 = jnp.float32, jnp.bfloat16

    order = [(db, du) for db in sorted(range(nb), key=lambda d: -min(d, nb - d)) for du in range(nu) if db + du > 0]
    others = []
    for db, du in order:
        tb, tu = lax.rem(blk + db, nb), lax.rem(uly + du, nu)
        others.append((tb * nu + tu, {"blk": tb, "uly": tu}))
    peers = [lax.rem(uly + du, nu) for du in range(1, nu)]

    raw = pltpu.make_async_copy(qkv, qkv_raw, local_sem.at[0])
    raw.start()
    patch_all[...] = jnp.zeros_like(patch_all)
    barrier = pltpu.get_barrier_semaphore()
    for _, target in others:
        pl.semaphore_signal(barrier, inc=1, device_id=target, device_id_type=MESH)

    lift_own = pltpu.make_async_copy(lift_w, lift_all.at[uly], local_sem.at[1])
    lift_own.start()
    loads = [
        pltpu.make_async_copy(a, b, local_sem.at[2 + i])
        for i, (a, b) in enumerate(((out_w, out_v), (sel, sel_v), (keep, keep_v)))
    ]
    conv_loads = [
        pltpu.make_async_copy(conv_w.at[layer], conv_v.at[layer], local_sem.at[5 + layer]) for layer in range(LAYERS)
    ]
    for copy in loads + conv_loads:
        copy.start()
    raw.wait()
    qkv_wide[...] = qkv_raw[...].astype(f32)
    heads = nd * hp
    for part in range(3):
        for head in range(heads):
            tokens = qkv_wide[pl.ds(part * heads + head, count, stride=3 * heads), :]
            qkv_mine[head // hp, part, head % hp] = tokens.astype(bf16)
    pl.semaphore_wait(barrier, nd - 1)

    sent = []
    for where, target in others:
        copy = remote(qkv_mine.at[where], qkv_all.at[me], q_send.at[where], q_recv.at[me], target)
        copy.start()
        sent.append(copy)
    for peer in peers:
        copy = remote(lift_w, lift_all.at[uly], l_send.at[peer], l_recv.at[uly], {"uly": peer})
        copy.start()
        sent.append(copy)
    qkv_all[me] = qkv_mine[me]
    for where, target in others:
        remote(qkv_mine.at[where], qkv_all.at[where], q_send.at[where], q_recv.at[where], target).wait_recv()

    scale = 1.0 / size**0.5
    for head in range(hp):
        q, k, v = (
            qkv_all[:, part, head].astype(f32).reshape(nd * count, size).astype(bf16) for part in range(3)
        )
        scores = lax.dot_general(q, k, NT, preferred_element_type=f32) * scale
        weights = jnp.exp(scores - jnp.max(scores, axis=1, keepdims=True))
        totals = jnp.sum(weights, axis=1, keepdims=True)
        mixed = jnp.dot(weights.astype(bf16), v, preferred_element_type=f32) / totals
        att_mine[:, :, head * size : (head + 1) * size] = mixed.reshape(nd, count, size).astype(bf16)

    for where, target in others:
        copy = remote(att_mine.at[where], att_all.at[me], a_send.at[where], a_recv.at[me], target)
        copy.start()
        sent.append(copy)

    for copy in loads:
        copy.wait()
    total = jnp.dot(att_mine[me], out_v[me], preferred_element_type=f32)
    for where, target in reversed(others):
        remote(att_mine.at[where], att_all.at[where], a_send.at[where], a_recv.at[where], target).wait_recv()
        total = total + jnp.dot(att_all[where], out_v[where], preferred_element_type=f32)
    patch = total.astype(bf16)
    patch_mine[...] = patch
    patch_all[1, uly] = patch

    def patch_copy(db, tu, slot, lane):
        return remote(
            patch_mine, patch_all.at[slot, lane], p_send.at[db + 1, tu], p_recv.at[slot, lane],
            {"blk": blk + db, "uly": tu},
        )

    reach = ((-1, blk > 0), (1, blk < nb - 1))
    for db, inside in reach:

        @pl.when(inside)
        def _():
            for tu in range(nu):
                patch_copy(db, tu, 1 - db, uly).start()

    for peer in peers:
        copy = remote(patch_mine, patch_all.at[1, uly], p_send.at[1, peer], p_recv.at[1, uly], {"uly": peer})
        copy.start()
        sent.append(copy)
    lift_own.wait()
    for peer in peers:
        remote(lift_w, lift_all.at[peer], l_send.at[peer], l_recv.at[peer], {"uly": peer}).wait_recv()
    lift = jnp.concatenate([lift_all[u] for u in range(nu)], axis=1)
    lift = jnp.concatenate([lift] * (PATCH * PATCH), axis=0)
    for peer in peers:
        remote(
            patch_mine, patch_all.at[1, peer], p_send.at[1, peer], p_recv.at[1, peer], {"uly": peer}
        ).wait_recv()
    for db, inside in reach:

        @pl.when(inside)
        def _():
            for tu in range(nu):
                copy = patch_copy(db, tu, 1 + db, tu)
                copy.wait_recv()
                copy.wait_send()

    patches = patch_all[...].astype(f32).reshape(-1, patch_all.shape[-1]).astype(bf16)
    spread = jnp.dot(sel_v[...], patches, preferred_element_type=f32).astype(bf16) * keep_v[...]
    x0[...] = jnp.dot(spread, lift, preferred_element_type=f32).astype(bf16)

    for layer in range(LAYERS):
        edge = LAYERS - 1 - layer
        conv_loads[layer].wait()
        cuts = plan(layer, own + 2 * edge)
        before = plan(layer - 1, own + 2 * edge + 2)
        ready = 0
        for chunk in range(len(cuts) - 1):
            base, span = cuts[chunk] * width, (cuts[chunk + 1] - cuts[chunk]) * width
            if layer > 0:
                while before[ready] < cuts[chunk + 1] + 2:
                    rows = slice(before[ready] * width, before[ready + 1] * width)
                    for peer in peers:
                        part = acts[layer - 1].at[peer, rows]
                        remote(
                            part, part, c_send.at[layer - 1, ready, peer], c_recv.at[layer - 1, ready, peer],
                            {"uly": peer},
                        ).wait_recv()
                    ready += 1
            acc = None
            for above in range(3):
                rows = slice(base + above * width, base + above * width + span)
                if layer == 0:
                    window = x0[rows, :]
                else:
                    window = jnp.concatenate([acts[layer - 1][u, rows, :] for u in range(nu)], axis=1)
                part = lax.dot_general(window, conv_v[layer, above], NT, preferred_element_type=f32)
                acc = part if acc is None else acc + part
            outs = acc.shape[1] // 3
            place = lax.broadcasted_iota(jnp.int32, (span, outs), 0)
            column = place & (width - 1)
            left = jnp.where(column == 0, 0.0, pltpu.roll(acc[:, :outs], 1, 0))
            right = jnp.where(column == width - 1, 0.0, pltpu.roll(acc[:, 2 * outs :], span - 1, 0))
            z = acc[:, outs : 2 * outs] + left + right
            y = z / (1.0 + jnp.exp(-z))
            if edge == 0:
                out[base : base + span, :] = y.astype(bf16)
                continue
            place = place + (base + (blk * own - edge) * width)
            y = jnp.where((place >= 0) & (place < nb * own * width), y, 0.0).astype(bf16)
            rows = slice(base, base + span)
            acts[layer][uly, rows, :] = y
            for peer in peers:
                part = acts[layer].at[uly, rows]
                copy = remote(
                    part, part, c_send.at[layer, chunk, peer], c_recv.at[layer, chunk, uly], {"uly": peer}
                )
                copy.start()
                sent.append(copy)

    for copy in sent:
        copy.wait_send()


def spread_tables(nu, rows, cols, latent_ch):
    own = PATCH * rows
    width = PATCH * cols * nu
    y, w = np.meshgrid(np.arange(own - LAYERS, 2 * own + LAYERS), np.arange(width), indexing="ij")
    y, w = y.reshape(-1), w.reshape(-1)
    slot, row = np.divmod(y // PATCH, rows)
    lane, col = np.divmod(w // PATCH, cols)
    token = ((slot * nu + lane) * rows + row) * cols + col
    sel = token[:, None] == np.arange(3 * nu * rows * cols)[None]
    piece = (y % PATCH) * PATCH + w % PATCH
    keep = piece[:, None] == (np.arange(PATCH * PATCH * latent_ch) // latent_ch)[None]
    return jnp.asarray(sel, jnp.bfloat16), jnp.asarray(keep, jnp.bfloat16)


def body_fused(nb, nu, qkv, out_weight, lift_weight, conv_weight):
    _, rows, cols, _, heads, size = qkv.shape
    nd, count = nb * nu, rows * cols
    hp = heads // nd
    own, width = PATCH * rows, PATCH * cols * nu
    most = 2
    latent_ch, outs = lift_weight.shape
    channels = conv_weight.shape[4]
    feats = out_weight.shape[1]
    tokens = qkv.reshape(count * 3 * heads, size)
    sel, keep = spread_tables(nu, rows, cols, latent_ch)
    bf16 = jnp.bfloat16
    dma = pltpu.SemaphoreType.DMA
    anywhere = pl.BlockSpec(memory_space=pl.ANY)
    pixels = pl.pallas_call(
        functools.partial(fused_kernel, (nb, nu, hp, size, own, width)),
        out_shape=pltpu.VMEM((own * width, outs), bf16),
        in_specs=[anywhere] * 6,
        out_specs=pl.BlockSpec(memory_space=pltpu.VMEM),
        scratch_shapes=[
            pltpu.VMEM(tokens.shape, bf16),
            pltpu.VMEM(tokens.shape, jnp.float32),
            pltpu.VMEM((nd, 3, hp, count, size), bf16),
            pltpu.VMEM((nd, 3, hp, count, size), bf16),
            pltpu.VMEM((nd, hp * size, feats), bf16),
            pltpu.VMEM((nu, latent_ch, outs), bf16),
            pltpu.VMEM((LAYERS, 3, 3 * outs, channels), bf16),
            pltpu.VMEM(sel.shape, bf16),
            pltpu.VMEM(keep.shape, bf16),
            pltpu.VMEM((nd, count, hp * size), bf16),
            pltpu.VMEM((nd, count, hp * size), bf16),
            pltpu.VMEM((count, feats), bf16),
            pltpu.VMEM((3, nu, count, feats), bf16),
            pltpu.VMEM(((own + 2 * LAYERS) * width, channels), bf16),
            [
                pltpu.VMEM((nu, (own + 2 * (LAYERS - 1 - layer)) * width, outs), bf16)
                for layer in range(LAYERS - 1)
            ],
            dma((5 + LAYERS,)),
            dma((nd,)), dma((nd,)), dma((nu,)), dma((nu,)), dma((nd,)), dma((nd,)),
            dma((3, nu)), dma((3, nu)), dma((LAYERS - 1, most, nu)), dma((LAYERS - 1, most, nu)),
        ],
        compiler_params=pltpu.CompilerParams(
            collective_id=0, has_side_effects=True, vmem_limit_bytes=60 * 1024 * 1024
        ),
    )(
        tokens,
        out_weight.reshape(nd, hp * size, feats),
        lift_weight,
        conv_weight.reshape(LAYERS, 3, 3 * outs, channels),
        sel,
        keep,
    )
    return pixels.reshape(1, own, width, outs)


def body(nb, nu, qkv, out_weight, lift_weight, conv_weight):
    frames, rows, cols, _, heads, size = qkv.shape
    width = PATCH * cols * nu
    fits = (
        frames == 1
        and nb > 1
        and nu > 1
        and heads % (nb * nu) == 0
        and (rows * cols) % 8 == 0
        and size % 128 == 0
        and lift_weight.shape[1] % 128 == 0
        and PATCH * rows >= LAYERS
        and width % 16 == 0
        and width & (width - 1) == 0
    )
    if fits:
        return body_fused(nb, nu, qkv, out_weight, lift_weight, conv_weight)
    return body_by_steps(qkv, out_weight, lift_weight, conv_weight)


def solution(mesh):
    in_specs = (
        P("grp", "blk", "uly", None, None, None),
        P(),
        P(None, "uly"),
        P(None, None, None, "uly", None),
    )
    out_specs = P("grp", "blk", None, "uly")
    step = functools.partial(body, mesh.shape["blk"], mesh.shape["uly"])
    return jax.shard_map(step, mesh=mesh, in_specs=in_specs, out_specs=out_specs, check_vma=False)
```
